32 devices in a mesh: blk: 16 (over z, x, core), rep: 2 (over y).
Axes of the slice: x: 2, y: 2, z: 4, core: 2. Of those that a mesh axis runs over, the one named last changes fastest.
Arguments:
- prices: float32 [512], replicated, may hold values from 0.5 to 1.5
- capacity: float32 [512], replicated, may hold values from -8 to 8
- coupling: bfloat16 [48, 32, 512], P(None, 'blk', 'rep'), may hold values from -0.25 to 0.25
- assign: int32 [65536], P(('blk', 'rep')), may hold values from 0 to 31
- avail: int32 [48, 65536], P(None, ('blk', 'rep')), may hold values 0 or 1
- agent_cap: float32 [65536], P(('blk', 'rep')), may hold values from 0.5 to 2
- value: float32 [48, 65536], P(None, ('blk', 'rep')), may hold values from -6 to 6
- weight: float32 [48, 65536], P(None, ('blk', 'rep')), may hold values from 0.5 to 2
- warm: float32 [48, 65536], P(None, ('blk', 'rep')), may hold values from 0 to 2
Outputs:
- plan: float32 [48, 65536], P(None, ('blk', 'rep'))
- new_prices: float32 [512], replicated
The draws below stay inside these ranges and needn't reach their ends.
All inputs are finite; a program needn't handle non-finite values. No bound on the sum of `avail` on one device may be relied on, other than what follows from the above.
Results may differ from the reference program's by a relative error of at most 0.0003.
Values may be sent and summed in bfloat16 or wider, within the bound.
A program may use at most 64 MiB of HBM per device.

```python
import math
import jax
import jax.numpy as jnp
from jax import lax

HORIZON = 48
CONSTRAINTS = 512
INNER = 8
FEEDERS = 32
AGENTS = 65536


def plant(entries, stream_key, smallest, high):
    longest = entries.shape.index(max(entries.shape))
    spots = []
    for shift in (0, 1):
        where = [jax.random.randint(jax.random.fold_in(stream_key, axis), (), 0, length) for axis, length in enumerate(entries.shape)]
        where[longest] = (where[longest] + shift) % entries.shape[longest]
        spots.append(tuple(where))
    return entries.at[spots[0]].set(smallest).at[spots[1]].set(high)


def level_of(stream_key, dims, split, smallest, high):
    def one(position, parts):
        draws = jax.random.uniform(jax.random.fold_in(jax.random.fold_in(stream_key, 6), position), (parts,), jnp.float32, smallest / len(split), high / len(split))
        return jnp.repeat(jnp.exp(draws), dims[position] // parts).reshape((-1,) + (1,) * (len(dims) - position - 1))

    factor_of = one(*split[0])
    for cut in split[1:]:
        factor_of = factor_of * one(*cut)
    return factor_of


def scatter_about(key, dims, deviation, most, split=(), held_as=jnp.bfloat16):
    entries = deviation * jax.random.normal(key, dims, jnp.float32)
    if split:
        entries = entries * level_of(key, dims, split, -0.22, 0.18)
    return jnp.clip(entries, -most, most).astype(held_as)


def setup_inputs(seed: int = 0) -> dict:
    key_list = jax.random.split(jax.random.key(seed), 10)
    prices = jnp.clip(jax.random.uniform(key_list[0], (CONSTRAINTS,), jnp.float32, 0.5, 1.5), 0.5, 1.5)
    capacity = scatter_about(key_list[1], (CONSTRAINTS,), 2.0, 8.0, (), jnp.float32)
    coupling = scatter_about(key_list[2], (HORIZON, FEEDERS, CONSTRAINTS), CONSTRAINTS ** -0.5, 0.25, ((1, 16), (2, 2)))
    assign = plant(jax.random.randint(key_list[3], (AGENTS,), 0, FEEDERS), jax.random.fold_in(key_list[3], 1), 0, FEEDERS - 1).astype(jnp.int32)
    avail = plant((jax.random.randint(key_list[4], (HORIZON, AGENTS), 0, 4) < 3).astype(jnp.int32), jax.random.fold_in(key_list[4], 1), 0, 1)
    agent_cap = jnp.clip(jnp.exp(math.log(2.0) - 1.3862944 * jax.random.uniform(key_list[5], (AGENTS,), jnp.float32) ** level_of(key_list[5], (AGENTS,), ((0, 32),), -0.2, 0.2)), 0.5, 2.0)
    value = scatter_about(key_list[6], (HORIZON, AGENTS), 1.0, 6.0, ((1, 32),), jnp.float32)
    weight = jnp.clip(jnp.exp(math.log(2.0) - 1.3862944 * jax.random.uniform(key_list[7], (HORIZON, AGENTS), jnp.float32) ** level_of(key_list[7], (HORIZON, AGENTS), ((1, 32),), -0.2, 0.2)), 0.5, 2.0)
    warm = jnp.clip(2.0 * jax.random.uniform(key_list[8], (HORIZON, AGENTS), jnp.float32) ** level_of(key_list[8], (HORIZON, AGENTS), ((1, 32),), -0.2, 0.2), 0.0, 2.0)
    return {"prices": prices, "capacity": capacity, "coupling": coupling, "assign": assign, "avail": avail, "agent_cap": agent_cap, "value": value, "weight": weight, "warm": warm}


def smooth_of(plan_now):
    diffs = plan_now[1:] - plan_now[:-1]
    zero_row = jnp.zeros((1, plan_now.shape[1]), jnp.float32)
    return jnp.concatenate([zero_row, diffs], 0) - jnp.concatenate([diffs, zero_row], 0)


def reference(prices, capacity, coupling, assign, avail, agent_cap, value, weight, warm):
    coeffs = coupling.astype(jnp.float32)
    table = jnp.einsum("tfr,r->tf", coeffs, prices, precision=lax.Precision.HIGHEST)
    price = table[:, assign]
    upper = agent_cap[None, :] * avail.astype(jnp.float32)
    plan = jnp.clip(warm, 0.0, upper)
    for _ in range(INNER):
        gradient = weight * plan + 1.0 * smooth_of(plan) - value + price
        plan = jnp.clip(plan - 0.15 * gradient, 0.0, upper)
    loads = jax.ops.segment_sum(plan.T, assign, num_segments=FEEDERS).T * (FEEDERS / AGENTS)
    sums = jnp.einsum("tfr,tf->r", coeffs, loads, precision=lax.Precision.HIGHEST)
    new_prices = jnp.maximum(0.0, prices + 0.1 * (sums - capacity))
    return plan, new_prices
```

```python
import functools

import jax
import jax.numpy as jnp
from jax import lax
from jax.experimental import pallas as pl
from jax.experimental.pallas import tpu as pltpu
from jax.sharding import PartitionSpec as P

INNER = 8
STEP = 0.15
LANES = 128
BF16 = jnp.bfloat16
F32 = jnp.float32
MESH = pl.DeviceIdType.MESH


def three_rows(row):
    high = row.astype(BF16).astype(F32)
    rest = row - high
    mid = rest.astype(BF16).astype(F32)
    low = rest - mid
    zeros = jnp.zeros((5, row.shape[1]), F32)
    return jnp.concatenate([high, mid, low, zeros], 0).astype(BF16)


def pad_lanes(rows, width):
    if rows.shape[1] == width:
        return rows
    return jnp.concatenate(
        [rows, jnp.zeros((rows.shape[0], width - rows.shape[1]), F32)], 1
    )


def each_peer(blks, reps, my_blk, my_rep, action):
    if blks * reps <= 64:
        for db in range(blks):
            for dr in range(reps):
                if db or dr:
                    action(lax.rem(my_blk + db, blks), lax.rem(my_rep + dr, reps))
        return

    def one(k, _):
        action(lax.rem(my_blk + k // reps, blks), lax.rem(my_rep + k % reps, reps))
        return 0

    lax.fori_loop(1, blks * reps, one, 0)


def kernel(
    blks, reps, scale,
    prices_ref, capacity_ref, coup_ref, assign_ref, cap_ref, avail_hbm, value_hbm, weight_hbm, warm_hbm,
    plan_hbm, new_ref,
    avail, value, weight, warm, price, plan, split, onehot, coup,
    send_a, recv_a, send_b, recv_b, send_c, recv_c,
    in_sem, out_sem, send_sem, recv_sem,
):
    horizon, agents = warm.shape
    feed_local = coup_ref.shape[1]
    feeders = feed_local * blks
    half = coup_ref.shape[2]
    chunks = half // LANES
    my_blk, my_rep = lax.axis_index("blk"), lax.axis_index("rep")
    wide = send_a.shape[1]

    barrier = pltpu.get_barrier_semaphore()
    each_peer(
        blks, reps, my_blk, my_rep,
        lambda b, r: pl.semaphore_signal(
            barrier, inc=1, device_id={"blk": b, "rep": r}, device_id_type=MESH
        ),
    )
    fetches = [
        pltpu.make_async_copy(src, dst, in_sem.at[i])
        for i, (src, dst) in enumerate(
            ((warm_hbm, warm), (weight_hbm, weight), (value_hbm, value), (avail_hbm, avail))
        )
    ]
    for fetch in fetches:
        fetch.start()

    my_prices = prices_ref[pl.ds(my_rep * chunks, chunks), :]
    my_row = jnp.concatenate([my_prices[c : c + 1] for c in range(chunks)], 1)
    price_rows = three_rows(my_row)
    for j in range(feed_local):
        coup[j] = coup_ref[:, j, :]
        part = lax.dot_general(
            price_rows, coup[j], (((1,), (1,)), ((), ())), preferred_element_type=F32
        )
        send_a[j : j + 1, :] = pad_lanes(jnp.sum(part, 0, keepdims=True), wide)

    pl.semaphore_wait(barrier, blks * reps - 1)

    def exchange(phase, source_of, received):
        def start(b, r):
            pltpu.make_async_remote_copy(
                src_ref=source_of(b),
                dst_ref=received.at[my_rep * blks + my_blk],
                send_sem=send_sem.at[phase],
                recv_sem=recv_sem.at[phase],
                device_id={"blk": b, "rep": r},
                device_id_type=MESH,
            ).start()

        each_peer(blks, reps, my_blk, my_rep, start)

    def arrived(phase, received):
        others = received.at[pl.ds(0, blks * reps - 1)]
        pltpu.make_async_copy(others, others, recv_sem.at[phase]).wait()

    def left(phase, received):
        others = received.at[pl.ds(0, blks * reps - 1)]
        pltpu.make_async_copy(others, others, send_sem.at[phase]).wait()

    exchange(0, lambda b: send_a, recv_a)
    recv_a[my_rep * blks + my_blk] = send_a[...]

    row = lax.broadcasted_iota(jnp.int32, (feeders, agents), 0)
    feeder = lax.rem(row, blks) * feed_local + row // blks
    hot = jnp.where(feeder == assign_ref[...], 1.0, 0.0).astype(BF16)
    for part in range(3):
        onehot[part * feeders : (part + 1) * feeders, :] = hot
    for fetch in fetches:
        fetch.wait()

    arrived(0, recv_a)
    rows = []
    for j in range(feed_local):
        total = recv_a[pl.ds(0, blks), j, :]
        for r in range(1, reps):
            total = total + recv_a[pl.ds(r * blks, blks), j, :]
        rows.append(total)
    table = jnp.concatenate(rows, 0).T[:horizon]
    high = table.astype(BF16).astype(F32)
    mid = (table - high).astype(BF16).astype(F32)
    low = table - high - mid
    table3 = jnp.concatenate([high, mid, low], 1).astype(BF16)
    price[...] = jnp.dot(table3, onehot[...], preferred_element_type=F32)

    step_row = lax.broadcasted_iota(jnp.int32, (horizon, LANES), 0)
    ends = jnp.where((step_row == 0) | (step_row == horizon - 1), 1.0, 2.0)
    zero_row = jnp.zeros((1, LANES), F32)
    for c in range(agents // LANES):
        at = pl.ds(c * LANES, LANES)
        upper = cap_ref[:, at] * avail[:, at].astype(F32)
        now = jnp.clip(warm[:, at], 0.0, upper)
        keep = 1.0 - STEP * (weight[:, at] + ends)
        push = STEP * (value[:, at] - price[:, at])
        for _ in range(INNER):
            near = jnp.concatenate([zero_row, now[:-1]], 0) + jnp.concatenate([now[1:], zero_row], 0)
            now = jnp.clip(keep * now + (push + STEP * near), 0.0, upper)
        plan[:, at] = now
        coarse = now.astype(BF16)
        split[:horizon, at] = coarse
        split[horizon:, at] = (now - coarse.astype(F32)).astype(BF16)
    put = pltpu.make_async_copy(plan, plan_hbm, out_sem)
    put.start()

    both = lax.dot_general(
        onehot[:feeders, :], split[...], (((1,), (1,)), ((), ())), preferred_element_type=F32
    )
    loads = pad_lanes((both[:, :horizon] + both[:, horizon:]) * scale, wide)
    for j in range(feed_local):
        send_b[:, j, :] = loads[j * blks : (j + 1) * blks]
    exchange(1, lambda b: send_b.at[b], recv_b)
    recv_b[my_rep * blks + my_blk] = send_b[my_blk]
    arrived(1, recv_b)
    my_loads = jnp.sum(recv_b[...], 0)

    sums = jnp.zeros((8, half), F32)
    for j in range(feed_local):
        sums = sums + jnp.dot(
            three_rows(my_loads[j : j + 1, :horizon]), coup[j], preferred_element_type=F32
        )
    sums = jnp.sum(sums, 0, keepdims=True)
    for c in range(chunks):
        send_c[c : c + 1, :] = sums[:, c * LANES : (c + 1) * LANES]
    exchange(2, lambda b: send_c, recv_c)
    recv_c[my_rep * blks + my_blk] = send_c[...]
    arrived(2, recv_c)
    for r in range(reps):
        total = jnp.sum(recv_c[pl.ds(r * blks, blks)], 0)
        mine = pl.ds(r * chunks, chunks)
        new_ref[mine, :] = jnp.maximum(
            0.0, prices_ref[mine, :] + 0.1 * (total - capacity_ref[mine, :])
        )
    left(0, recv_a)
    left(1, recv_b)
    left(2, recv_c)
    put.wait()


def solution(mesh):
    blks, reps = mesh.shape["blk"], mesh.shape["rep"]

    def shards(prices, capacity, coupling, assign, avail, agent_cap, value, weight, warm):
        horizon, agents = warm.shape
        feed_local, half = coupling.shape[1:]
        feeders = feed_local * blks
        devices = blks * reps
        constraints = prices.shape[0]
        wide = -(-horizon // LANES) * LANES
        vmem = pl.BlockSpec(memory_space=pltpu.VMEM)
        hbm = pl.BlockSpec(memory_space=pl.ANY)
        rows = (constraints // LANES, LANES)
        plan, new_prices = pl.pallas_call(
            functools.partial(kernel, blks, reps, feeders / (agents * devices)),
            out_shape=(
                jax.ShapeDtypeStruct((horizon, agents), F32),
                jax.ShapeDtypeStruct(rows, F32),
            ),
            in_specs=[vmem] * 5 + [hbm] * 4,
            out_specs=(hbm, vmem),
            scratch_shapes=[
                pltpu.VMEM((horizon, agents), jnp.int32),
                pltpu.VMEM((horizon, agents), F32),
                pltpu.VMEM((horizon, agents), F32),
                pltpu.VMEM((horizon, agents), F32),
                pltpu.VMEM((horizon, agents), F32),
                pltpu.VMEM((horizon, agents), F32),
                pltpu.VMEM((2 * horizon, agents), BF16),
                pltpu.VMEM((3 * feeders, agents), BF16),
                pltpu.VMEM((feed_local, horizon, half), BF16),
                pltpu.VMEM((feed_local, wide), F32),
                pltpu.VMEM((devices, feed_local, wide), F32),
                pltpu.VMEM((blks, feed_local, wide), F32),
                pltpu.VMEM((devices, feed_local, wide), F32),
                pltpu.VMEM((half // LANES, LANES), F32),
                pltpu.VMEM((devices, half // LANES, LANES), F32),
                pltpu.SemaphoreType.DMA((4,)),
                pltpu.SemaphoreType.DMA,
                pltpu.SemaphoreType.DMA((3,)),
                pltpu.SemaphoreType.DMA((3,)),
            ],
            compiler_params=pltpu.CompilerParams(collective_id=0, has_side_effects=True),
        )(
            prices.reshape(rows), capacity.reshape(rows), coupling,
            assign.reshape(1, agents), agent_cap.reshape(1, agents),
            avail, value, weight, warm,
        )
        return plan, new_prices.reshape(constraints)

    placed = (
        P(),
        P(),
        P(None, "blk", "rep"),
        P(("blk", "rep")),
        P(None, ("blk", "rep")),
        P(("blk", "rep")),
        P(None, ("blk", "rep")),
        P(None, ("blk", "rep")),
        P(None, ("blk", "rep")),
    )
    return jax.shard_map(
        shards,
        mesh=mesh,
        in_specs=placed,
        out_specs=(P(None, ("blk", "rep")), P()),
        check_vma=False,
    )
```

```python
import functools

import jax
import jax.numpy as jnp
from jax import lax
from jax.experimental import pallas as pl
from jax.experimental.pallas import tpu as pltpu
from jax.sharding import PartitionSpec as P

INNER = 8
STEP = 0.15
LANES = 128
BF16 = jnp.bfloat16
F32 = jnp.float32
MESH = pl.DeviceIdType.MESH


def three_rows(row):
    high = row.astype(BF16).astype(F32)
    rest = row - high
    mid = rest.astype(BF16).astype(F32)
    low = rest - mid
    zeros = jnp.zeros((5, row.shape[1]), F32)
    return jnp.concatenate([high, mid, low, zeros], 0).astype(BF16)


def pad_lanes(rows, width):
    if rows.shape[1] == width:
        return rows
    return jnp.concatenate(
        [rows, jnp.zeros((rows.shape[0], width - rows.shape[1]), F32)], 1
    )


def each_peer(blks, reps, my_blk, my_rep, action):
    if blks * reps <= 64:
        for db in range(blks):
            for dr in range(reps):
                if db or dr:
                    action(lax.rem(my_blk + db, blks), lax.rem(my_rep + dr, reps))
        return

    def one(k, _):
        action(lax.rem(my_blk + k // reps, blks), lax.rem(my_rep + k % reps, reps))
        return 0

    lax.fori_loop(1, blks * reps, one, 0)


def group_count(blks):
    return 4 if blks % 4 == 0 else 1


def kernel(
    blks, reps, scale,
    prices_hbm, capacity_hbm, coup_hbm, assign_hbm, cap_hbm, avail_hbm, value_hbm, weight_hbm, warm_hbm,
    plan, new_ref,
    prices, capacity, raw, assign, cap, avail, value, weight, warm, price, split, table_hot, load_hot, coup,
    send_a, recv_a, send_b, recv_b, send_c, recv_c,
    in_sem, send_sem, recv_sem,
):
    horizon, agents = warm.shape
    feed_local, half = raw.shape[1:]
    feeders = feed_local * blks
    chunks = half // LANES
    groups = group_count(blks)
    members = blks // groups
    held = groups * feed_local
    my_blk, my_rep = lax.axis_index("blk"), lax.axis_index("rep")
    my_group, my_member = my_blk // members, lax.rem(my_blk, members)
    me = my_rep * blks + my_blk
    wide = send_a.shape[1]

    barrier = pltpu.get_barrier_semaphore()
    each_peer(
        blks, reps, my_blk, my_rep,
        lambda b, r: pl.semaphore_signal(
            barrier, inc=1, device_id={"blk": b, "rep": r}, device_id_type=MESH
        ),
    )
    fetches = [
        pltpu.make_async_copy(src, dst, in_sem.at[i])
        for i, (src, dst) in enumerate(
            (
                (prices_hbm, prices), (coup_hbm, raw), (assign_hbm, assign), (cap_hbm, cap),
                (warm_hbm, warm), (weight_hbm, weight), (value_hbm, value), (avail_hbm, avail),
                (capacity_hbm, capacity),
            )
        )
    ]
    for fetch in fetches:
        fetch.start()
    fetches[0].wait()
    fetches[1].wait()

    my_prices = prices[pl.ds(my_rep * chunks, chunks), :]
    my_row = jnp.concatenate([my_prices[c : c + 1] for c in range(chunks)], 1)
    price_rows = three_rows(my_row)
    for j in range(feed_local):
        mine = raw[:, j, :]
        coup[my_group, j] = mine
        part = lax.dot_general(
            price_rows, mine, (((1,), (1,)), ((), ())), preferred_element_type=F32
        )
        send_a[j : j + 1, :] = pad_lanes(jnp.sum(part, 0, keepdims=True), wide)

    pl.semaphore_wait(barrier, blks * reps - 1)

    def send(phase, source, target, b, r):
        pltpu.make_async_remote_copy(
            src_ref=source,
            dst_ref=target,
            send_sem=send_sem.at[phase],
            recv_sem=recv_sem.at[phase],
            device_id={"blk": b, "rep": r},
            device_id_type=MESH,
        ).start()

    def wait_for(sem, received):
        others = received.at[pl.ds(0, received.shape[0] - 1)]
        pltpu.make_async_copy(others, others, sem).wait()

    each_peer(blks, reps, my_blk, my_rep, lambda b, r: send(0, send_a, recv_a.at[me], b, r))
    for dg in range(1, groups):
        there = lax.rem(my_group + dg, groups) * members + my_member
        send(3, coup.at[my_group], coup.at[my_group], there, my_rep)
    recv_a[me] = send_a[...]

    fetches[2].wait()
    row = lax.broadcasted_iota(jnp.int32, (feeders, agents), 0)
    feeder = lax.rem(row, blks) * feed_local + row // blks
    hot = jnp.where(feeder == assign[...], 1.0, 0.0).astype(BF16)
    for part in range(3):
        table_hot[part * feeders : (part + 1) * feeders, :] = hot
    slot = row // members
    feeder = ((slot // feed_local) * members + lax.rem(row, members)) * feed_local + lax.rem(
        slot, feed_local
    )
    load_hot[...] = jnp.where(feeder == assign[...], 1.0, 0.0).astype(BF16)
    for fetch in fetches[3:]:
        fetch.wait()

    wait_for(recv_sem.at[0], recv_a)
    rows = []
    for j in range(feed_local):
        total = recv_a[pl.ds(0, blks), j, :]
        for r in range(1, reps):
            total = total + recv_a[pl.ds(r * blks, blks), j, :]
        rows.append(total)
    table = jnp.concatenate(rows, 0).T[:horizon]
    high = table.astype(BF16).astype(F32)
    mid = (table - high).astype(BF16).astype(F32)
    low = table - high - mid
    table3 = jnp.concatenate([high, mid, low], 1).astype(BF16)
    price[...] = jnp.dot(table3, table_hot[...], preferred_element_type=F32)

    step_row = lax.broadcasted_iota(jnp.int32, (horizon, LANES), 0)
    ends = jnp.where((step_row == 0) | (step_row == horizon - 1), 1.0, 2.0)
    zero_row = jnp.zeros((1, LANES), F32)
    for c in range(agents // LANES):
        at = pl.ds(c * LANES, LANES)
        upper = cap[:, at] * avail[:, at].astype(F32)
        now = jnp.clip(warm[:, at], 0.0, upper)
        keep = 1.0 - STEP * (weight[:, at] + ends)
        push = STEP * (value[:, at] - price[:, at])
        for _ in range(INNER):
            near = jnp.concatenate([zero_row, now[:-1]], 0) + jnp.concatenate([now[1:], zero_row], 0)
            now = jnp.clip(keep * now + (push + STEP * near), 0.0, upper)
        plan[:, at] = now
        coarse = now.astype(BF16)
        split[:horizon, at] = coarse
        split[horizon:, at] = (now - coarse.astype(F32)).astype(BF16)

    both = lax.dot_general(
        load_hot[...], split[...], (((1,), (1,)), ((), ())), preferred_element_type=F32
    )
    loads = pad_lanes((both[:, :horizon] + both[:, horizon:]) * scale, wide)
    for q in range(held):
        send_b[:, q, :] = loads[q * members : (q + 1) * members]
    my_seat = my_rep * members + my_member

    def send_loads(m, r):
        send(1, send_b.at[m], recv_b.at[my_seat], my_group * members + m, r)

    each_peer(members, reps, my_member, my_rep, send_loads)
    recv_b[my_seat] = send_b[my_member]
    wait_for(recv_sem.at[1], recv_b)
    group_loads = jnp.sum(recv_b[...], 0)[:, :horizon]
    if groups > 1:
        wait_for(recv_sem.at[3], coup)

    high = group_loads.astype(BF16).astype(F32)
    mid = (group_loads - high).astype(BF16).astype(F32)
    low = group_loads - high - mid
    stack = jnp.concatenate([high, mid, low, jnp.zeros_like(low)], 0)
    owner = lax.rem(lax.broadcasted_iota(jnp.int32, stack.shape, 0), held)
    sums = jnp.zeros((4 * held, half), F32)
    for q in range(held):
        sums = sums + jnp.dot(
            jnp.where(owner == q, stack, 0.0).astype(BF16),
            coup[q // feed_local, q % feed_local],
            preferred_element_type=F32,
        )
    sums = jnp.sum(sums, 0, keepdims=True)
    for c in range(chunks):
        send_c[c : c + 1, :] = sums[:, c * LANES : (c + 1) * LANES]
    each_peer(blks, reps, my_blk, my_rep, lambda b, r: send(2, send_c, recv_c.at[me], b, r))
    recv_c[me] = send_c[...]
    wait_for(recv_sem.at[2], recv_c)
    for r in range(reps):
        total = jnp.sum(recv_c[pl.ds(r * blks, blks)], 0)
        here = pl.ds(r * chunks, chunks)
        new_ref[here, :] = jnp.maximum(
            0.0, prices[here, :] + 0.1 * (total - capacity[here, :])
        )
    wait_for(send_sem.at[0], recv_a)
    wait_for(send_sem.at[1], recv_b)
    wait_for(send_sem.at[2], recv_c)
    if groups > 1:
        wait_for(send_sem.at[3], coup)


def solution(mesh):
    blks, reps = mesh.shape["blk"], mesh.shape["rep"]
    groups = group_count(blks)
    members = blks // groups

    def shards(prices, capacity, coupling, assign, avail, agent_cap, value, weight, warm):
        horizon, agents = warm.shape
        feed_local, half = coupling.shape[1:]
        feeders = feed_local * blks
        devices = blks * reps
        constraints = prices.shape[0]
        wide = -(-horizon // LANES) * LANES
        vmem = pl.BlockSpec(memory_space=pltpu.VMEM)
        hbm = pl.BlockSpec(memory_space=pl.ANY)
        rows = (constraints // LANES, LANES)
        whole = (horizon, agents)
        plan, new_prices = pl.pallas_call(
            functools.partial(kernel, blks, reps, feeders / (agents * devices)),
            out_shape=(pltpu.VMEM(whole, F32), pltpu.VMEM(rows, F32)),
            in_specs=[hbm] * 9,
            out_specs=(vmem, vmem),
            scratch_shapes=[
                pltpu.VMEM(rows, F32),
                pltpu.VMEM(rows, F32),
                pltpu.VMEM(coupling.shape, BF16),
                pltpu.VMEM((1, agents), jnp.int32),
                pltpu.VMEM((1, agents), F32),
                pltpu.VMEM(whole, jnp.int32),
                pltpu.VMEM(whole, F32),
                pltpu.VMEM(whole, F32),
                pltpu.VMEM(whole, F32),
                pltpu.VMEM(whole, F32),
                pltpu.VMEM((2 * horizon, agents), BF16),
                pltpu.VMEM((3 * feeders, agents), BF16),
                pltpu.VMEM((feeders, agents), BF16),
                pltpu.VMEM((groups, feed_local, horizon, half), BF16),
                pltpu.VMEM((feed_local, wide), F32),
                pltpu.VMEM((devices, feed_local, wide), F32),
                pltpu.VMEM((members, groups * feed_local, wide), F32),
                pltpu.VMEM((members * reps, groups * feed_local, wide), F32),
                pltpu.VMEM((half // LANES, LANES), F32),
                pltpu.VMEM((devices, half // LANES, LANES), F32),
                pltpu.SemaphoreType.DMA((9,)),
                pltpu.SemaphoreType.DMA((4,)),
                pltpu.SemaphoreType.DMA((4,)),
            ],
            compiler_params=pltpu.CompilerParams(collective_id=0, has_side_effects=True),
        )(
            prices.reshape(rows), capacity.reshape(rows), coupling,
            assign.reshape(1, agents), agent_cap.reshape(1, agents),
            avail, value, weight, warm,
        )
        return plan, new_prices.reshape(constraints)

    placed = (
        P(),
        P(),
        P(None, "blk", "rep"),
        P(("blk", "rep")),
        P(None, ("blk", "rep")),
        P(("blk", "rep")),
        P(None, ("blk", "rep")),
        P(None, ("blk", "rep")),
        P(None, ("blk", "rep")),
    )
    return jax.shard_map(
        shards,
        mesh=mesh,
        in_specs=placed,
        out_specs=(P(None, ("blk", "rep")), P()),
        check_vma=False,
    )
```

```python
import functools

import jax
import jax.numpy as jnp
from jax import lax
from jax.experimental import pallas as pl
from jax.experimental.pallas import tpu as pltpu
from jax.sharding import PartitionSpec as P

INNER = 8
STEP = 0.15
LANES = 128
BLOCK = 256
EIGHT = 8
BF16 = jnp.bfloat16
F32 = jnp.float32
MESH = pl.DeviceIdType.MESH


def three_rows(row):
    high = row.astype(BF16).astype(F32)
    rest = row - high
    mid = rest.astype(BF16).astype(F32)
    low = rest - mid
    zeros = jnp.zeros((5, row.shape[1]), F32)
    return jnp.concatenate([high, mid, low, zeros], 0).astype(BF16)


def pad_lanes(rows, width):
    if rows.shape[1] == width:
        return rows
    return jnp.concatenate(
        [rows, jnp.zeros((rows.shape[0], width - rows.shape[1]), F32)], 1
    )


def each_peer(blks, reps, my_blk, my_rep, action):
    if blks * reps <= 64:
        for db in range(blks):
            for dr in range(reps):
                if db or dr:
                    action(lax.rem(my_blk + db, blks), lax.rem(my_rep + dr, reps))
        return

    def one(k, _):
        action(lax.rem(my_blk + k // reps, blks), lax.rem(my_rep + k % reps, reps))
        return 0

    lax.fori_loop(1, blks * reps, one, 0)


def group_count(blks):
    return 4 if blks % 4 == 0 else 1


def kernel(
    blks, reps, scale,
    prices_hbm, capacity_hbm, coup_hbm, assign_hbm, cap_hbm, avail_hbm, value_hbm, weight_hbm, warm_hbm,
    plan, new_ref,
    prices, capacity, raw, stage, assign, cap, avail, value, weight, warm, start, upper, keep, push, done, table_hot, load_hot, coup,
    send_a, recv_a, send_b, recv_b, send_c, recv_c,
    in_sem, out_sem, send_sem, recv_sem,
):
    blocks, horizon = warm.shape[:2]
    agents = blocks * LANES
    feed_local, half = raw.shape[1:]
    feeders = feed_local * blks
    strides = horizon // EIGHT
    chunks = half // LANES
    groups = group_count(blks)
    members = blks // groups
    held = groups * feed_local
    my_blk, my_rep = lax.axis_index("blk"), lax.axis_index("rep")
    my_group, my_member = my_blk // members, lax.rem(my_blk, members)
    me = my_rep * blks + my_blk
    wide = send_a.shape[1]

    barrier = pltpu.get_barrier_semaphore()
    each_peer(
        blks, reps, my_blk, my_rep,
        lambda b, r: pl.semaphore_signal(
            barrier, inc=1, device_id={"blk": b, "rep": r}, device_id_type=MESH
        ),
    )
    fetches = [
        pltpu.make_async_copy(src, dst, in_sem.at[i])
        for i, (src, dst) in enumerate(
            (
                (prices_hbm, prices), (coup_hbm, raw), (assign_hbm, assign), (cap_hbm, cap),
                (capacity_hbm, capacity),
            )
        )
    ]
    for fetch in fetches:
        fetch.start()
    tiled = ((warm_hbm, warm), (weight_hbm, weight), (value_hbm, value), (avail_hbm, avail))
    for i, (src, dst) in enumerate(tiled):
        for c in range(agents // LANES):
            pltpu.make_async_copy(
                src.at[:, pl.ds(c * LANES, LANES)], dst.at[c], in_sem.at[5 + i]
            ).start()
    fetches[0].wait()
    fetches[1].wait()

    my_prices = prices[pl.ds(my_rep * chunks, chunks), :]
    my_row = jnp.concatenate([my_prices[c : c + 1] for c in range(chunks)], 1)
    price_rows = three_rows(my_row)
    for j in range(feed_local):
        natural = raw[:, j, :].astype(F32)
        for c in range(chunks):
            stage[c] = natural[:, c * LANES : (c + 1) * LANES]
        mine = jnp.concatenate(
            [
                jnp.concatenate(
                    [stage[c, pl.ds(v, EIGHT, stride=strides), :] for v in range(strides)], 0
                )
                for c in range(chunks)
            ],
            1,
        ).astype(BF16)
        coup[my_group, j] = mine
        part = lax.dot_general(
            price_rows, mine, (((1,), (1,)), ((), ())), preferred_element_type=F32
        )
        send_a[j : j + 1, :] = pad_lanes(jnp.sum(part, 0, keepdims=True), wide)

    pl.semaphore_wait(barrier, blks * reps - 1)

    def send(phase, source, target, b, r):
        pltpu.make_async_remote_copy(
            src_ref=source,
            dst_ref=target,
            send_sem=send_sem.at[phase],
            recv_sem=recv_sem.at[phase],
            device_id={"blk": b, "rep": r},
            device_id_type=MESH,
        ).start()

    def wait_for(sem, received):
        others = received.at[pl.ds(0, received.shape[0] - 1)]
        pltpu.make_async_copy(others, others, sem).wait()

    each_peer(blks, reps, my_blk, my_rep, lambda b, r: send(0, send_a, recv_a.at[me], b, r))
    for dg in range(1, groups):
        there = lax.rem(my_group + dg, groups) * members + my_member
        send(3, coup.at[my_group], coup.at[my_group], there, my_rep)
    recv_a[me] = send_a[...]

    fetches[2].wait()
    row = lax.broadcasted_iota(jnp.int32, (feeders, agents), 0)
    feeder = lax.rem(row, blks) * feed_local + row // blks
    hot = jnp.where(feeder == assign[...], 1.0, 0.0).astype(BF16)
    for part in range(3):
        table_hot[part * feeders : (part + 1) * feeders, :] = hot
    slot = row // members
    feeder = ((slot // feed_local) * members + lax.rem(row, members)) * feed_local + lax.rem(
        slot, feed_local
    )
    load_hot[...] = jnp.where(feeder == assign[...], 1.0, 0.0).astype(BF16)
    for fetch in fetches[3:]:
        fetch.wait()
    for i, (_, dst) in enumerate(tiled):
        pltpu.make_async_copy(dst, dst, in_sem.at[5 + i]).wait()

    eighth = lax.broadcasted_iota(jnp.int32, (EIGHT, LANES), 0)
    first, last = eighth == 0, eighth == EIGHT - 1
    for c in range(agents // LANES):
        at = pl.ds(c * LANES, LANES)
        for v in range(strides):
            there = pl.ds(v, EIGHT, stride=strides)
            here = pl.ds(v * EIGHT, EIGHT)
            limit = cap[:, at] * avail[c, there, :].astype(F32)
            near = jnp.full((EIGHT, LANES), 2.0, F32)
            if v == 0:
                near = near - jnp.where(first, 1.0, 0.0)
            if v == strides - 1:
                near = near - jnp.where(last, 1.0, 0.0)
            upper[here, at] = limit
            start[here, at] = jnp.clip(warm[c, there, :], 0.0, limit)
            keep[here, at] = 1.0 - STEP * (weight[c, there, :] + near)
            push[here, at] = STEP * value[c, there, :]

    wait_for(recv_sem.at[0], recv_a)
    rows = []
    for j in range(feed_local):
        total = recv_a[pl.ds(0, blks), j, :]
        for r in range(1, reps):
            total = total + recv_a[pl.ds(r * blks, blks), j, :]
        rows.append(total)
    table = jnp.concatenate(rows, 0).T[:horizon]
    high = table.astype(BF16).astype(F32)
    mid = (table - high).astype(BF16).astype(F32)
    low = table - high - mid
    table3 = jnp.concatenate([high, mid, low], 1).astype(BF16)

    both = jnp.zeros((feeders, 2 * horizon), F32)
    for c in range(agents // BLOCK):
        block = pl.ds(c * BLOCK, BLOCK)
        price = STEP * jnp.dot(table3, table_hot[:, block], preferred_element_type=F32)
        parts = []
        for d in range(BLOCK // LANES):
            at = pl.ds(c * BLOCK + d * LANES, LANES)
            rows = [slice(v * EIGHT, (v + 1) * EIGHT) for v in range(strides)]
            now = [start[row, at] for row in rows]
            most = [upper[row, at] for row in rows]
            held_back = [keep[row, at] for row in rows]
            drive = [
                push[row, at] - price[row, d * LANES : (d + 1) * LANES] for row in rows
            ]
            for _ in range(INNER):
                before = jnp.where(first, 0.0, pltpu.roll(now[-1], 1, 0))
                after = jnp.where(last, 0.0, pltpu.roll(now[0], EIGHT - 1, 0))
                line = [before] + now + [after]
                now = [
                    jnp.clip(
                        held_back[v] * now[v] + (drive[v] + STEP * (line[v] + line[v + 2])),
                        0.0, most[v],
                    )
                    for v in range(strides)
                ]
            for v in range(strides):
                done[c * (BLOCK // LANES) + d, pl.ds(v, EIGHT, stride=strides), :] = now[v]
            now = jnp.concatenate(now, 0)
            coarse = now.astype(BF16).astype(F32)
            parts.append(jnp.concatenate([coarse, now - coarse], 0).astype(BF16))
        both = both + lax.dot_general(
            load_hot[:, block], jnp.concatenate(parts, 1), (((1,), (1,)), ((), ())),
            preferred_element_type=F32,
        )
    for c in range(blocks):
        pltpu.make_async_copy(done.at[c], plan.at[:, pl.ds(c * LANES, LANES)], out_sem).start()
    loads = pad_lanes((both[:, :horizon] + both[:, horizon:]) * scale, wide)
    for q in range(held):
        send_b[:, q, :] = loads[q * members : (q + 1) * members]
    my_seat = my_rep * members + my_member

    def send_loads(m, r):
        send(1, send_b.at[m], recv_b.at[my_seat], my_group * members + m, r)

    each_peer(members, reps, my_member, my_rep, send_loads)
    recv_b[my_seat] = send_b[my_member]
    wait_for(recv_sem.at[1], recv_b)
    group_loads = jnp.sum(recv_b[...], 0)[:, :horizon]
    if groups > 1:
        wait_for(recv_sem.at[3], coup)

    high = group_loads.astype(BF16).astype(F32)
    mid = (group_loads - high).astype(BF16).astype(F32)
    low = group_loads - high - mid
    stack = jnp.concatenate([high, mid, low, jnp.zeros_like(low)], 0)
    owner = lax.rem(lax.broadcasted_iota(jnp.int32, stack.shape, 0), held)
    sums = jnp.zeros((4 * held, half), F32)
    for q in range(held):
        sums = sums + jnp.dot(
            jnp.where(owner == q, stack, 0.0).astype(BF16),
            coup[q // feed_local, q % feed_local],
            preferred_element_type=F32,
        )
    sums = jnp.sum(sums, 0, keepdims=True)
    for c in range(chunks):
        send_c[c : c + 1, :] = sums[:, c * LANES : (c + 1) * LANES]
    each_peer(blks, reps, my_blk, my_rep, lambda b, r: send(2, send_c, recv_c.at[me], b, r))
    recv_c[me] = send_c[...]
    wait_for(recv_sem.at[2], recv_c)
    for r in range(reps):
        total = jnp.sum(recv_c[pl.ds(r * blks, blks)], 0)
        here = pl.ds(r * chunks, chunks)
        new_ref[here, :] = jnp.maximum(
            0.0, prices[here, :] + 0.1 * (total - capacity[here, :])
        )
    pltpu.make_async_copy(done, done, out_sem).wait()
    wait_for(send_sem.at[0], recv_a)
    wait_for(send_sem.at[1], recv_b)
    wait_for(send_sem.at[2], recv_c)
    if groups > 1:
        wait_for(send_sem.at[3], coup)


def solution(mesh):
    blks, reps = mesh.shape["blk"], mesh.shape["rep"]
    groups = group_count(blks)
    members = blks // groups

    def shards(prices, capacity, coupling, assign, avail, agent_cap, value, weight, warm):
        horizon, agents = warm.shape
        feed_local, half = coupling.shape[1:]
        feeders = feed_local * blks
        devices = blks * reps
        constraints = prices.shape[0]
        wide = -(-horizon // LANES) * LANES
        vmem = pl.BlockSpec(memory_space=pltpu.VMEM)
        hbm = pl.BlockSpec(memory_space=pl.ANY)
        rows = (constraints // LANES, LANES)
        whole = (horizon, agents)
        tiles = (agents // LANES, horizon, LANES)
        plan, new_prices = pl.pallas_call(
            functools.partial(kernel, blks, reps, feeders / (agents * devices)),
            out_shape=(pltpu.VMEM(whole, F32), pltpu.VMEM(rows, F32)),
            in_specs=[hbm] * 9,
            out_specs=(vmem, vmem),
            scratch_shapes=[
                pltpu.VMEM(rows, F32),
                pltpu.VMEM(rows, F32),
                pltpu.VMEM(coupling.shape, BF16),
                pltpu.VMEM((half // LANES, horizon, LANES), F32),
                pltpu.VMEM((1, agents), jnp.int32),
                pltpu.VMEM((1, agents), F32),
                pltpu.VMEM(tiles, jnp.int32),
                pltpu.VMEM(tiles, F32),
                pltpu.VMEM(tiles, F32),
                pltpu.VMEM(tiles, F32),
                pltpu.VMEM(whole, F32),
                pltpu.VMEM(whole, F32),
                pltpu.VMEM(whole, F32),
                pltpu.VMEM(whole, F32),
                pltpu.VMEM(tiles, F32),
                pltpu.VMEM((3 * feeders, agents), BF16),
                pltpu.VMEM((feeders, agents), BF16),
                pltpu.VMEM((groups, feed_local, horizon, half), BF16),
                pltpu.VMEM((feed_local, wide), F32),
                pltpu.VMEM((devices, feed_local, wide), F32),
                pltpu.VMEM((members, groups * feed_local, wide), F32),
                pltpu.VMEM((members * reps, groups * feed_local, wide), F32),
                pltpu.VMEM((half // LANES, LANES), F32),
                pltpu.VMEM((devices, half // LANES, LANES), F32),
                pltpu.SemaphoreType.DMA((9,)),
                pltpu.SemaphoreType.DMA,
                pltpu.SemaphoreType.DMA((4,)),
                pltpu.SemaphoreType.DMA((4,)),
            ],
            compiler_params=pltpu.CompilerParams(collective_id=0, has_side_effects=True),
        )(
            prices.reshape(rows), capacity.reshape(rows), coupling,
            assign.reshape(1, agents), agent_cap.reshape(1, agents),
            avail, value, weight, warm,
        )
        return plan, new_prices.reshape(constraints)

    placed = (
        P(),
        P(),
        P(None, "blk", "rep"),
        P(("blk", "rep")),
        P(None, ("blk", "rep")),
        P(("blk", "rep")),
        P(None, ("blk", "rep")),
        P(None, ("blk", "rep")),
        P(None, ("blk", "rep")),
    )
    return jax.shard_map(
        shards,
        mesh=mesh,
        in_specs=placed,
        out_specs=(P(None, ("blk", "rep")), P()),
        check_vma=False,
    )
```

```python
import functools

import jax
import jax.numpy as jnp
from jax import lax
from jax.experimental import pallas as pl
from jax.experimental.pallas import tpu as pltpu
from jax.sharding import PartitionSpec as P

INNER = 8
STEP = 0.15
LANES = 128
BLOCK = 256
EIGHT = 8
BF16 = jnp.bfloat16
F32 = jnp.float32
MESH = pl.DeviceIdType.MESH


def three_rows(row):
    high = row.astype(BF16).astype(F32)
    rest = row - high
    mid = rest.astype(BF16).astype(F32)
    low = rest - mid
    zeros = jnp.zeros((5, row.shape[1]), F32)
    return jnp.concatenate([high, mid, low, zeros], 0).astype(BF16)


def pad_lanes(rows, width):
    if rows.shape[1] == width:
        return rows
    return jnp.concatenate(
        [rows, jnp.zeros((rows.shape[0], width - rows.shape[1]), F32)], 1
    )


def each_peer(blks, reps, my_blk, my_rep, action):
    if blks * reps <= 64:
        groups = group_count(blks)
        members = blks // groups
        my_group, my_member = my_blk // members, lax.rem(my_blk, members)
        far_first = sorted(range(groups), key=lambda dg: (dg == 0, -abs(2 * dg - groups)))
        for dg in far_first:
            group = lax.rem(my_group + dg, groups) * members
            for dm in reversed(range(members)):
                for dr in reversed(range(reps)):
                    if dg or dm or dr:
                        action(
                            group + lax.rem(my_member + dm, members), lax.rem(my_rep + dr, reps)
                        )
        return

    def one(k, _):
        action(lax.rem(my_blk + k // reps, blks), lax.rem(my_rep + k % reps, reps))
        return 0

    lax.fori_loop(1, blks * reps, one, 0)


def group_count(blks):
    return 4 if blks % 4 == 0 else 1


def kernel(
    blks, reps, scale,
    prices_hbm, capacity_hbm, coup_hbm, assign_hbm, cap_hbm, avail_hbm, value_hbm, weight_hbm, warm_hbm,
    plan, new_ref,
    prices, capacity, raw, stage, assign, cap, avail, value, weight, warm, start, upper, keep, push, done, table_hot, load_hot, coup,
    send_a, recv_a, send_b, recv_b, send_c, recv_c,
    in_sem, out_sem, send_sem, recv_sem,
):
    blocks, horizon = warm.shape[:2]
    agents = blocks * LANES
    feed_local, half = raw.shape[1:]
    feeders = feed_local * blks
    strides = horizon // EIGHT
    chunks = half // LANES
    groups = group_count(blks)
    members = blks // groups
    held = groups * feed_local
    my_blk, my_rep = lax.axis_index("blk"), lax.axis_index("rep")
    my_group, my_member = my_blk // members, lax.rem(my_blk, members)
    me = my_rep * blks + my_blk
    wide = send_a.shape[1]

    barrier = pltpu.get_barrier_semaphore()
    each_peer(
        blks, reps, my_blk, my_rep,
        lambda b, r: pl.semaphore_signal(
            barrier, inc=1, device_id={"blk": b, "rep": r}, device_id_type=MESH
        ),
    )
    fetches = [
        pltpu.make_async_copy(src, dst, in_sem.at[i])
        for i, (src, dst) in enumerate(
            (
                (prices_hbm, prices), (coup_hbm, raw), (assign_hbm, assign), (cap_hbm, cap),
                (capacity_hbm, capacity),
            )
        )
    ]
    for fetch in fetches:
        fetch.start()
    tiled = ((warm_hbm, warm), (weight_hbm, weight), (value_hbm, value), (avail_hbm, avail))
    for i, (src, dst) in enumerate(tiled):
        for c in range(agents // LANES):
            pltpu.make_async_copy(
                src.at[:, pl.ds(c * LANES, LANES)], dst.at[c], in_sem.at[5 + i]
            ).start()
    fetches[0].wait()
    fetches[1].wait()

    my_prices = prices[pl.ds(my_rep * chunks, chunks), :]
    my_row = jnp.concatenate([my_prices[c : c + 1] for c in range(chunks)], 1)
    price_rows = three_rows(my_row)
    for j in range(feed_local):
        natural = raw[:, j, :].astype(F32)
        for c in range(chunks):
            stage[c] = natural[:, c * LANES : (c + 1) * LANES]
        mine = jnp.concatenate(
            [
                jnp.concatenate(
                    [stage[c, pl.ds(v, EIGHT, stride=strides), :] for v in range(strides)], 0
                )
                for c in range(chunks)
            ],
            1,
        ).astype(BF16)
        coup[my_group, j] = mine
        part = lax.dot_general(
            price_rows, mine, (((1,), (1,)), ((), ())), preferred_element_type=F32
        )
        send_a[j : j + 1, :] = pad_lanes(jnp.sum(part, 0, keepdims=True), wide)

    pl.semaphore_wait(barrier, blks * reps - 1)

    def send(phase, source, target, b, r):
        pltpu.make_async_remote_copy(
            src_ref=source,
            dst_ref=target,
            send_sem=send_sem.at[phase],
            recv_sem=recv_sem.at[phase],
            device_id={"blk": b, "rep": r},
            device_id_type=MESH,
        ).start()

    def wait_for(sem, received):
        others = received.at[pl.ds(0, received.shape[0] - 1)]
        pltpu.make_async_copy(others, others, sem).wait()

    each_peer(blks, reps, my_blk, my_rep, lambda b, r: send(0, send_a, recv_a.at[me], b, r))
    for dg in range(1, groups):
        there = lax.rem(my_group + dg, groups) * members + my_member
        send(3, coup.at[my_group], coup.at[my_group], there, my_rep)
    recv_a[me] = send_a[...]

    fetches[2].wait()
    row = lax.broadcasted_iota(jnp.int32, (feeders, agents), 0)
    feeder = lax.rem(row, blks) * feed_local + row // blks
    hot = jnp.where(feeder == assign[...], 1.0, 0.0).astype(BF16)
    for part in range(3):
        table_hot[part * feeders : (part + 1) * feeders, :] = hot
    slot = row // members
    feeder = ((slot // feed_local) * members + lax.rem(row, members)) * feed_local + lax.rem(
        slot, feed_local
    )
    load_hot[...] = jnp.where(feeder == assign[...], 1.0, 0.0).astype(BF16)
    for fetch in fetches[3:]:
        fetch.wait()
    for i, (_, dst) in enumerate(tiled):
        pltpu.make_async_copy(dst, dst, in_sem.at[5 + i]).wait()

    eighth = lax.broadcasted_iota(jnp.int32, (EIGHT, LANES), 0)
    first, last = eighth == 0, eighth == EIGHT - 1
    for c in range(agents // LANES):
        at = pl.ds(c * LANES, LANES)
        for v in range(strides):
            there = pl.ds(v, EIGHT, stride=strides)
            here = pl.ds(v * EIGHT, EIGHT)
            limit = cap[:, at] * avail[c, there, :].astype(F32)
            near = jnp.full((EIGHT, LANES), 2.0, F32)
            if v == 0:
                near = near - jnp.where(first, 1.0, 0.0)
            if v == strides - 1:
                near = near - jnp.where(last, 1.0, 0.0)
            upper[here, at] = limit
            start[here, at] = jnp.clip(warm[c, there, :], 0.0, limit)
            keep[here, at] = 1.0 - STEP * (weight[c, there, :] + near)
            push[here, at] = STEP * value[c, there, :]

    wait_for(recv_sem.at[0], recv_a)
    rows = []
    for j in range(feed_local):
        total = recv_a[pl.ds(0, blks), j, :]
        for r in range(1, reps):
            total = total + recv_a[pl.ds(r * blks, blks), j, :]
        rows.append(total)
    table = jnp.concatenate(rows, 0).T[:horizon]
    high = table.astype(BF16).astype(F32)
    mid = (table - high).astype(BF16).astype(F32)
    low = table - high - mid
    table3 = jnp.concatenate([high, mid, low], 1).astype(BF16)

    both = jnp.zeros((feeders, 2 * horizon), F32)
    for c in range(agents // BLOCK):
        block = pl.ds(c * BLOCK, BLOCK)
        price = STEP * jnp.dot(table3, table_hot[:, block], preferred_element_type=F32)
        parts = []
        for d in range(BLOCK // LANES):
            at = pl.ds(c * BLOCK + d * LANES, LANES)
            rows = [slice(v * EIGHT, (v + 1) * EIGHT) for v in range(strides)]
            now = [start[row, at] for row in rows]
            most = [upper[row, at] for row in rows]
            held_back = [keep[row, at] for row in rows]
            drive = [
                push[row, at] - price[row, d * LANES : (d + 1) * LANES] for row in rows
            ]
            for _ in range(INNER):
                before = jnp.where(first, 0.0, pltpu.roll(now[-1], 1, 0))
                after = jnp.where(last, 0.0, pltpu.roll(now[0], EIGHT - 1, 0))
                line = [before] + now + [after]
                now = [
                    jnp.clip(
                        held_back[v] * now[v] + (drive[v] + STEP * (line[v] + line[v + 2])),
                        0.0, most[v],
                    )
                    for v in range(strides)
                ]
            for v in range(strides):
                done[c * (BLOCK // LANES) + d, pl.ds(v, EIGHT, stride=strides), :] = now[v]
            now = jnp.concatenate(now, 0)
            coarse = now.astype(BF16).astype(F32)
            parts.append(jnp.concatenate([coarse, now - coarse], 0).astype(BF16))
        both = both + lax.dot_general(
            load_hot[:, block], jnp.concatenate(parts, 1), (((1,), (1,)), ((), ())),
            preferred_element_type=F32,
        )
    for c in range(blocks):
        pltpu.make_async_copy(done.at[c], plan.at[:, pl.ds(c * LANES, LANES)], out_sem).start()
    loads = pad_lanes((both[:, :horizon] + both[:, horizon:]) * scale, wide)
    for q in range(held):
        send_b[:, q, :] = loads[q * members : (q + 1) * members]
    my_seat = my_rep * members + my_member

    def send_loads(m, r):
        send(1, send_b.at[m], recv_b.at[my_seat], my_group * members + m, r)

    each_peer(members, reps, my_member, my_rep, send_loads)
    recv_b[my_seat] = send_b[my_member]
    wait_for(recv_sem.at[1], recv_b)
    group_loads = jnp.sum(recv_b[...], 0)[:, :horizon]
    if groups > 1:
        wait_for(recv_sem.at[3], coup)

    high = group_loads.astype(BF16).astype(F32)
    mid = (group_loads - high).astype(BF16).astype(F32)
    low = group_loads - high - mid
    stack = jnp.concatenate([high, mid, low, jnp.zeros_like(low)], 0)
    owner = lax.rem(lax.broadcasted_iota(jnp.int32, stack.shape, 0), held)
    sums = jnp.zeros((4 * held, half), F32)
    for q in range(held):
        sums = sums + jnp.dot(
            jnp.where(owner == q, stack, 0.0).astype(BF16),
            coup[q // feed_local, q % feed_local],
            preferred_element_type=F32,
        )
    sums = jnp.sum(sums, 0, keepdims=True)
    for c in range(chunks):
        send_c[c : c + 1, :] = sums[:, c * LANES : (c + 1) * LANES]
    each_peer(blks, reps, my_blk, my_rep, lambda b, r: send(2, send_c, recv_c.at[me], b, r))
    recv_c[me] = send_c[...]
    wait_for(recv_sem.at[2], recv_c)
    for r in range(reps):
        total = jnp.sum(recv_c[pl.ds(r * blks, blks)], 0)
        here = pl.ds(r * chunks, chunks)
        new_ref[here, :] = jnp.maximum(
            0.0, prices[here, :] + 0.1 * (total - capacity[here, :])
        )
    pltpu.make_async_copy(done, done, out_sem).wait()
    wait_for(send_sem.at[0], recv_a)
    wait_for(send_sem.at[1], recv_b)
    wait_for(send_sem.at[2], recv_c)
    if groups > 1:
        wait_for(send_sem.at[3], coup)


def solution(mesh):
    blks, reps = mesh.shape["blk"], mesh.shape["rep"]
    groups = group_count(blks)
    members = blks // groups

    def shards(prices, capacity, coupling, assign, avail, agent_cap, value, weight, warm):
        horizon, agents = warm.shape
        feed_local, half = coupling.shape[1:]
        feeders = feed_local * blks
        devices = blks * reps
        constraints = prices.shape[0]
        wide = -(-horizon // LANES) * LANES
        vmem = pl.BlockSpec(memory_space=pltpu.VMEM)
        hbm = pl.BlockSpec(memory_space=pl.ANY)
        rows = (constraints // LANES, LANES)
        whole = (horizon, agents)
        tiles = (agents // LANES, horizon, LANES)
        plan, new_prices = pl.pallas_call(
            functools.partial(kernel, blks, reps, feeders / (agents * devices)),
            out_shape=(pltpu.VMEM(whole, F32), pltpu.VMEM(rows, F32)),
            in_specs=[hbm] * 9,
            out_specs=(vmem, vmem),
            scratch_shapes=[
                pltpu.VMEM(rows, F32),
                pltpu.VMEM(rows, F32),
                pltpu.VMEM(coupling.shape, BF16),
                pltpu.VMEM((half // LANES, horizon, LANES), F32),
                pltpu.VMEM((1, agents), jnp.int32),
                pltpu.VMEM((1, agents), F32),
                pltpu.VMEM(tiles, jnp.int32),
                pltpu.VMEM(tiles, F32),
                pltpu.VMEM(tiles, F32),
                pltpu.VMEM(tiles, F32),
                pltpu.VMEM(whole, F32),
                pltpu.VMEM(whole, F32),
                pltpu.VMEM(whole, F32),
                pltpu.VMEM(whole, F32),
                pltpu.VMEM(tiles, F32),
                pltpu.VMEM((3 * feeders, agents), BF16),
                pltpu.VMEM((feeders, agents), BF16),
                pltpu.VMEM((groups, feed_local, horizon, half), BF16),
                pltpu.VMEM((feed_local, wide), F32),
                pltpu.VMEM((devices, feed_local, wide), F32),
                pltpu.VMEM((members, groups * feed_local, wide), F32),
                pltpu.VMEM((members * reps, groups * feed_local, wide), F32),
                pltpu.VMEM((half // LANES, LANES), F32),
                pltpu.VMEM((devices, half // LANES, LANES), F32),
                pltpu.SemaphoreType.DMA((9,)),
                pltpu.SemaphoreType.DMA,
                pltpu.SemaphoreType.DMA((4,)),
                pltpu.SemaphoreType.DMA((4,)),
            ],
            compiler_params=pltpu.CompilerParams(collective_id=0, has_side_effects=True),
        )(
            prices.reshape(rows), capacity.reshape(rows), coupling,
            assign.reshape(1, agents), agent_cap.reshape(1, agents),
            avail, value, weight, warm,
        )
        return plan, new_prices.reshape(constraints)

    placed = (
        P(),
        P(),
        P(None, "blk", "rep"),
        P(("blk", "rep")),
        P(None, ("blk", "rep")),
        P(("blk", "rep")),
        P(None, ("blk", "rep")),
        P(None, ("blk", "rep")),
        P(None, ("blk", "rep")),
    )
    return jax.shard_map(
        shards,
        mesh=mesh,
        in_specs=placed,
        out_specs=(P(None, ("blk", "rep")), P()),
        check_vma=False,
    )
```

```python
import functools

import jax
import jax.numpy as jnp
from jax import lax
from jax.experimental import pallas as pl
from jax.experimental.pallas import tpu as pltpu
from jax.sharding import PartitionSpec as P

INNER = 8
STEP = 0.15
LANES = 128
BLOCK = 256
EIGHT = 8
BF16 = jnp.bfloat16
F32 = jnp.float32
MESH = pl.DeviceIdType.MESH


def three_rows(row):
    high = row.astype(BF16).astype(F32)
    rest = row - high
    mid = rest.astype(BF16).astype(F32)
    low = rest - mid
    zeros = jnp.zeros((5, row.shape[1]), F32)
    return jnp.concatenate([high, mid, low, zeros], 0).astype(BF16)


def pad_lanes(rows, width):
    if rows.shape[1] == width:
        return rows
    return jnp.concatenate(
        [rows, jnp.zeros((rows.shape[0], width - rows.shape[1]), F32)], 1
    )


def each_peer(blks, reps, my_blk, my_rep, action):
    if blks * reps <= 64:
        groups = group_count(blks)
        members = blks // groups
        my_group, my_member = my_blk // members, lax.rem(my_blk, members)
        far_first = sorted(range(groups), key=lambda dg: (dg == 0, -abs(2 * dg - groups)))
        for dg in far_first:
            group = lax.rem(my_group + dg, groups) * members
            for dm in reversed(range(members)):
                for dr in reversed(range(reps)):
                    if dg or dm or dr:
                        action(
                            group + lax.rem(my_member + dm, members), lax.rem(my_rep + dr, reps)
                        )
        return

    def one(k, _):
        action(lax.rem(my_blk + k // reps, blks), lax.rem(my_rep + k % reps, reps))
        return 0

    lax.fori_loop(1, blks * reps, one, 0)


def group_count(blks):
    return 4 if blks % 4 == 0 else 1


def kernel(
    blks, reps, scale,
    prices_hbm, capacity_hbm, coup_hbm, assign_hbm, cap_hbm, avail_hbm, value_hbm, weight_hbm, warm_hbm,
    plan, new_ref,
    prices, capacity, raw, stage, assign, cap, avail, value, weight, warm, start, upper, keep, push, done, table_hot, load_hot, coup,
    send_a, recv_a, send_b, recv_b, send_c, recv_c,
    in_sem, out_sem, send_sem, recv_sem,
):
    blocks, horizon = warm.shape[:2]
    agents = blocks * LANES
    feed_local, half = raw.shape[1:]
    feeders = feed_local * blks
    strides = horizon // EIGHT
    chunks = half // LANES
    groups = group_count(blks)
    members = blks // groups
    held = groups * feed_local
    my_blk, my_rep = lax.axis_index("blk"), lax.axis_index("rep")
    my_group, my_member = my_blk // members, lax.rem(my_blk, members)
    me = my_rep * blks + my_blk
    wide = send_a.shape[1]

    barrier = pltpu.get_barrier_semaphore()
    each_peer(
        blks, reps, my_blk, my_rep,
        lambda b, r: pl.semaphore_signal(
            barrier, inc=1, device_id={"blk": b, "rep": r}, device_id_type=MESH
        ),
    )
    fetches = [
        pltpu.make_async_copy(src, dst, in_sem.at[i])
        for i, (src, dst) in enumerate(
            (
                (prices_hbm, prices), (coup_hbm, raw), (assign_hbm, assign), (cap_hbm, cap),
                (capacity_hbm, capacity),
            )
        )
    ]
    for fetch in fetches:
        fetch.start()
    tiled = ((warm_hbm, warm), (weight_hbm, weight), (value_hbm, value), (avail_hbm, avail))
    for i, (src, dst) in enumerate(tiled):
        for c in range(agents // LANES):
            pltpu.make_async_copy(
                src.at[:, pl.ds(c * LANES, LANES)], dst.at[c], in_sem.at[5 + i]
            ).start()
    fetches[0].wait()
    fetches[1].wait()

    my_prices = prices[pl.ds(my_rep * chunks, chunks), :]
    my_row = jnp.concatenate([my_prices[c : c + 1] for c in range(chunks)], 1)
    price_rows = three_rows(my_row)
    for j in range(feed_local):
        natural = raw[:, j, :].astype(F32)
        for c in range(chunks):
            stage[c] = natural[:, c * LANES : (c + 1) * LANES]
        mine = jnp.concatenate(
            [
                jnp.concatenate(
                    [stage[c, pl.ds(v, EIGHT, stride=strides), :] for v in range(strides)], 0
                )
                for c in range(chunks)
            ],
            1,
        ).astype(BF16)
        coup[my_group, j] = mine
        part = lax.dot_general(
            price_rows, mine, (((1,), (1,)), ((), ())), preferred_element_type=F32
        )
        send_a[j : j + 1, :] = pad_lanes(jnp.sum(part, 0, keepdims=True), wide)

    pl.semaphore_wait(barrier, blks * reps - 1)

    def send(phase, source, target, b, r):
        pltpu.make_async_remote_copy(
            src_ref=source,
            dst_ref=target,
            send_sem=send_sem.at[phase],
            recv_sem=recv_sem.at[phase],
            device_id={"blk": b, "rep": r},
            device_id_type=MESH,
        ).start()

    def wait_for(sem, received):
        others = received.at[pl.ds(0, received.shape[0] - 1)]
        pltpu.make_async_copy(others, others, sem).wait()

    each_peer(blks, reps, my_blk, my_rep, lambda b, r: send(0, send_a, recv_a.at[me], b, r))
    recv_a[me] = send_a[...]

    fetches[2].wait()
    row = lax.broadcasted_iota(jnp.int32, (feeders, agents), 0)
    feeder = lax.rem(row, blks) * feed_local + row // blks
    hot = jnp.where(feeder == assign[...], 1.0, 0.0).astype(BF16)
    for part in range(3):
        table_hot[part * feeders : (part + 1) * feeders, :] = hot
    slot = row // members
    feeder = ((slot // feed_local) * members + lax.rem(row, members)) * feed_local + lax.rem(
        slot, feed_local
    )
    load_hot[...] = jnp.where(feeder == assign[...], 1.0, 0.0).astype(BF16)
    for fetch in fetches[3:]:
        fetch.wait()
    for i, (_, dst) in enumerate(tiled):
        pltpu.make_async_copy(dst, dst, in_sem.at[5 + i]).wait()

    eighth = lax.broadcasted_iota(jnp.int32, (EIGHT, LANES), 0)
    first, last = eighth == 0, eighth == EIGHT - 1
    for c in range(agents // LANES):
        at = pl.ds(c * LANES, LANES)
        for v in range(strides):
            there = pl.ds(v, EIGHT, stride=strides)
            here = pl.ds(v * EIGHT, EIGHT)
            limit = cap[:, at] * avail[c, there, :].astype(F32)
            near = jnp.full((EIGHT, LANES), 2.0, F32)
            if v == 0:
                near = near - jnp.where(first, 1.0, 0.0)
            if v == strides - 1:
                near = near - jnp.where(last, 1.0, 0.0)
            upper[here, at] = limit
            start[here, at] = jnp.clip(warm[c, there, :], 0.0, limit)
            keep[here, at] = 1.0 - STEP * (weight[c, there, :] + near)
            push[here, at] = STEP * value[c, there, :]

    wait_for(recv_sem.at[0], recv_a)
    for dg in range(1, groups):
        there = lax.rem(my_group + dg, groups) * members + my_member
        send(3, coup.at[my_group], coup.at[my_group], there, my_rep)
    rows = []
    for j in range(feed_local):
        total = recv_a[pl.ds(0, blks), j, :]
        for r in range(1, reps):
            total = total + recv_a[pl.ds(r * blks, blks), j, :]
        rows.append(total)
    table = jnp.concatenate(rows, 0).T[:horizon]
    high = table.astype(BF16).astype(F32)
    mid = (table - high).astype(BF16).astype(F32)
    low = table - high - mid
    table3 = jnp.concatenate([high, mid, low], 1).astype(BF16)

    both = jnp.zeros((feeders, 2 * horizon), F32)
    for c in range(agents // BLOCK):
        block = pl.ds(c * BLOCK, BLOCK)
        price = STEP * jnp.dot(table3, table_hot[:, block], preferred_element_type=F32)
        parts = []
        for d in range(BLOCK // LANES):
            at = pl.ds(c * BLOCK + d * LANES, LANES)
            rows = [slice(v * EIGHT, (v + 1) * EIGHT) for v in range(strides)]
            now = [start[row, at] for row in rows]
            most = [upper[row, at] for row in rows]
            held_back = [keep[row, at] for row in rows]
            drive = [
                push[row, at] - price[row, d * LANES : (d + 1) * LANES] for row in rows
            ]
            for _ in range(INNER):
                before = jnp.where(first, 0.0, pltpu.roll(now[-1], 1, 0))
                after = jnp.where(last, 0.0, pltpu.roll(now[0], EIGHT - 1, 0))
                line = [before] + now + [after]
                now = [
                    jnp.clip(
                        held_back[v] * now[v] + (drive[v] + STEP * (line[v] + line[v + 2])),
                        0.0, most[v],
                    )
                    for v in range(strides)
                ]
            for v in range(strides):
                done[c * (BLOCK // LANES) + d, pl.ds(v, EIGHT, stride=strides), :] = now[v]
            now = jnp.concatenate(now, 0)
            coarse = now.astype(BF16).astype(F32)
            parts.append(jnp.concatenate([coarse, now - coarse], 0).astype(BF16))
        both = both + lax.dot_general(
            load_hot[:, block], jnp.concatenate(parts, 1), (((1,), (1,)), ((), ())),
            preferred_element_type=F32,
        )
    for c in range(blocks):
        pltpu.make_async_copy(done.at[c], plan.at[:, pl.ds(c * LANES, LANES)], out_sem).start()
    loads = pad_lanes((both[:, :horizon] + both[:, horizon:]) * scale, wide)
    for q in range(held):
        send_b[:, q, :] = loads[q * members : (q + 1) * members]
    my_seat = my_rep * members + my_member

    def send_loads(m, r):
        send(1, send_b.at[m], recv_b.at[my_seat], my_group * members + m, r)

    each_peer(members, reps, my_member, my_rep, send_loads)
    recv_b[my_seat] = send_b[my_member]
    wait_for(recv_sem.at[1], recv_b)
    group_loads = jnp.sum(recv_b[...], 0)[:, :horizon]
    if groups > 1:
        wait_for(recv_sem.at[3], coup)

    high = group_loads.astype(BF16).astype(F32)
    mid = (group_loads - high).astype(BF16).astype(F32)
    low = group_loads - high - mid
    stack = jnp.concatenate([high, mid, low, jnp.zeros_like(low)], 0)
    owner = lax.rem(lax.broadcasted_iota(jnp.int32, stack.shape, 0), held)
    sums = jnp.zeros((4 * held, half), F32)
    for q in range(held):
        sums = sums + jnp.dot(
            jnp.where(owner == q, stack, 0.0).astype(BF16),
            coup[q // feed_local, q % feed_local],
            preferred_element_type=F32,
        )
    sums = jnp.sum(sums, 0, keepdims=True)
    for c in range(chunks):
        send_c[c : c + 1, :] = sums[:, c * LANES : (c + 1) * LANES]
    each_peer(blks, reps, my_blk, my_rep, lambda b, r: send(2, send_c, recv_c.at[me], b, r))
    recv_c[me] = send_c[...]
    wait_for(recv_sem.at[2], recv_c)
    for r in range(reps):
        total = jnp.sum(recv_c[pl.ds(r * blks, blks)], 0)
        here = pl.ds(r * chunks, chunks)
        new_ref[here, :] = jnp.maximum(
            0.0, prices[here, :] + 0.1 * (total - capacity[here, :])
        )
    pltpu.make_async_copy(done, done, out_sem).wait()
    wait_for(send_sem.at[0], recv_a)
    wait_for(send_sem.at[1], recv_b)
    wait_for(send_sem.at[2], recv_c)
    if groups > 1:
        wait_for(send_sem.at[3], coup)


def solution(mesh):
    blks, reps = mesh.shape["blk"], mesh.shape["rep"]
    groups = group_count(blks)
    members = blks // groups

    def shards(prices, capacity, coupling, assign, avail, agent_cap, value, weight, warm):
        horizon, agents = warm.shape
        feed_local, half = coupling.shape[1:]
        feeders = feed_local * blks
        devices = blks * reps
        constraints = prices.shape[0]
        wide = -(-horizon // LANES) * LANES
        vmem = pl.BlockSpec(memory_space=pltpu.VMEM)
        hbm = pl.BlockSpec(memory_space=pl.ANY)
        rows = (constraints // LANES, LANES)
        whole = (horizon, agents)
        tiles = (agents // LANES, horizon, LANES)
        plan, new_prices = pl.pallas_call(
            functools.partial(kernel, blks, reps, feeders / (agents * devices)),
            out_shape=(pltpu.VMEM(whole, F32), pltpu.VMEM(rows, F32)),
            in_specs=[hbm] * 9,
            out_specs=(vmem, vmem),
            scratch_shapes=[
                pltpu.VMEM(rows, F32),
                pltpu.VMEM(rows, F32),
                pltpu.VMEM(coupling.shape, BF16),
                pltpu.VMEM((half // LANES, horizon, LANES), F32),
                pltpu.VMEM((1, agents), jnp.int32),
                pltpu.VMEM((1, agents), F32),
                pltpu.VMEM(tiles, jnp.int32),
                pltpu.VMEM(tiles, F32),
                pltpu.VMEM(tiles, F32),
                pltpu.VMEM(tiles, F32),
                pltpu.VMEM(whole, F32),
                pltpu.VMEM(whole, F32),
                pltpu.VMEM(whole, F32),
                pltpu.VMEM(whole, F32),
                pltpu.VMEM(tiles, F32),
                pltpu.VMEM((3 * feeders, agents), BF16),
                pltpu.VMEM((feeders, agents), BF16),
                pltpu.VMEM((groups, feed_local, horizon, half), BF16),
                pltpu.VMEM((feed_local, wide), F32),
                pltpu.VMEM((devices, feed_local, wide), F32),
                pltpu.VMEM((members, groups * feed_local, wide), F32),
                pltpu.VMEM((members * reps, groups * feed_local, wide), F32),
                pltpu.VMEM((half // LANES, LANES), F32),
                pltpu.VMEM((devices, half // LANES, LANES), F32),
                pltpu.SemaphoreType.DMA((9,)),
                pltpu.SemaphoreType.DMA,
                pltpu.SemaphoreType.DMA((4,)),
                pltpu.SemaphoreType.DMA((4,)),
            ],
            compiler_params=pltpu.CompilerParams(collective_id=0, has_side_effects=True),
        )(
            prices.reshape(rows), capacity.reshape(rows), coupling,
            assign.reshape(1, agents), agent_cap.reshape(1, agents),
            avail, value, weight, warm,
        )
        return plan, new_prices.reshape(constraints)

    placed = (
        P(),
        P(),
        P(None, "blk", "rep"),
        P(("blk", "rep")),
        P(None, ("blk", "rep")),
        P(("blk", "rep")),
        P(None, ("blk", "rep")),
        P(None, ("blk", "rep")),
        P(None, ("blk", "rep")),
    )
    return jax.shard_map(
        shards,
        mesh=mesh,
        in_specs=placed,
        out_specs=(P(None, ("blk", "rep")), P()),
        check_vma=False,
    )
```
